32 devices in a mesh: replica: 4 (over y, core), model: 8 (over z, x).
Axes of the slice: x: 2, y: 2, z: 4, core: 2. Of those that a mesh axis runs over, the one named last changes fastest.
Arguments:
- partial_query: float32 [4, 2048, 2048], P('replica', None, 'model'), may hold values from -4 to 4
- partial_key: float32 [4, 2048, 2048], P('replica', None, 'model'), may hold values from -4 to 4
- partial_value: float32 [4, 2048, 2048], P('replica', None, 'model'), may hold values from -4 to 4
- partial_mixed: float32 [4, 2048, 2048], P('replica', 'model'), may hold values from -4 to 4
- partial_norm: float32 [4, 2048], P('replica'), may hold values from -8 to 8
- partial_bias: float32 [4, 2048], P('replica'), may hold values from -8 to 8
- master_query: float32 [2048, 2048], P('replica', 'model'), may hold values from -0.1875 to 0.1875
- master_key: float32 [2048, 2048], P('replica', 'model'), may hold values from -0.1875 to 0.1875
- master_value: float32 [2048, 2048], P('replica', 'model'), may hold values from -0.1875 to 0.1875
- master_mixed: float32 [2048, 2048], P('model', 'replica'), may hold values from -0.1875 to 0.1875
- master_norm: float32 [2048], P('replica'), may hold values from 0.25 to 1.75
- master_bias: float32 [2048], P('replica'), may hold values from -3 to 3
- memory_query: float32 [2048, 2048], P('replica', 'model'), may hold values from 9.765625e-05 to 0.0009765625
- memory_key: float32 [2048, 2048], P('replica', 'model'), may hold values from 9.765625e-05 to 0.0009765625
- memory_value: float32 [2048, 2048], P('replica', 'model'), may hold values from 9.765625e-05 to 0.0009765625
- memory_mixed: float32 [2048, 2048], P('model', 'replica'), may hold values from 9.765625e-05 to 0.0009765625
- memory_norm: float32 [2048], P('replica'), may hold values from 0.05 to 0.8
- memory_bias: float32 [2048], P('replica'), may hold values from 0.05 to 0.8
Outputs:
- compute_query: bfloat16 [2048, 2048], P(None, 'model')
- compute_key: bfloat16 [2048, 2048], P(None, 'model')
- compute_value: bfloat16 [2048, 2048], P(None, 'model')
- compute_mixed: bfloat16 [2048, 2048], P('model')
- compute_norm: bfloat16 [2048], replicated
- compute_bias: bfloat16 [2048], replicated
- stepped_query: float32 [2048, 2048], P('replica', 'model')
- stepped_key: float32 [2048, 2048], P('replica', 'model')
- stepped_value: float32 [2048, 2048], P('replica', 'model')
- stepped_mixed: float32 [2048, 2048], P('model', 'replica')
- stepped_norm: float32 [2048], P('replica')
- stepped_bias: float32 [2048], P('replica')
- state_new_query: float32 [2048, 2048], P('replica', 'model')
- state_new_key: float32 [2048, 2048], P('replica', 'model')
- state_new_value: float32 [2048, 2048], P('replica', 'model')
- state_new_mixed: float32 [2048, 2048], P('model', 'replica')
- state_new_norm: float32 [2048], P('replica')
- state_new_bias: float32 [2048], P('replica')
The draws below stay inside these ranges and needn't reach their ends.
All inputs are finite; a program needn't handle non-finite values.
Results may differ from the reference program's by a relative error of at most 0.0004.
Values may be sent and summed in bfloat16 or wider, within the bound.
A program may use at most 64 MiB of HBM per device.

```python
import jax
import jax.numpy as jnp
from jax import lax

WIDTH = 2048
ATTN = 2048
REPLICAS = 4


def with_spikes(drawn, stream_key, source, target, shards_of, factor):
    def block_of(axis_at):
        return (jnp.arange(drawn.shape[axis_at]) // (drawn.shape[axis_at] // shards_of)).reshape((-1,) + (1,) * (drawn.ndim - 1 - axis_at))

    first = jax.random.permutation(stream_key, shards_of)[block_of(target)]
    second = (block_of(target) + shards_of // 2) % shards_of
    return jnp.where((block_of(source) == first) | (block_of(source) == second), factor * drawn, drawn)


def block_scale(key, extent, split, smallest, high):
    gain, own = 1.0, jax.random.fold_in(key, 6)
    for dim, parts in split:
        draws = jnp.exp(jax.random.uniform(jax.random.fold_in(own, dim), (parts,), jnp.float32, smallest / len(split), high / len(split)))
        gain = gain * jnp.repeat(draws, extent[dim] // parts).reshape([-1 if axis == dim else 1 for axis in range(len(extent))])
    return gain


def noise(rng, shape, scale, reach, split=(), dtype=jnp.bfloat16):
    values = jax.random.normal(rng, shape, jnp.float32) * scale
    if len(split) > 0:
        values = block_scale(rng, shape, split, -0.22, 0.18) * values
    return jnp.clip(values, min=-reach, max=reach).astype(dtype)


def gaussian_with(own_key, dims, width, bound, pieces, heavy, held_as=jnp.bfloat16):
    array = width * jax.random.normal(own_key, dims, jnp.float32)
    if pieces:
        array = array * block_scale(own_key, dims, pieces, -0.22, 0.18)
    return jnp.clip(with_spikes(array, jax.random.fold_in(own_key, 3), *heavy), -bound, bound).astype(held_as)


def setup_inputs(seed: int = 0) -> dict:
    keys = jax.random.split(jax.random.key(seed), 19)
    return {
        "partial_query": gaussian_with(keys[0], (REPLICAS, WIDTH, ATTN), 0.5, 4.0, ((0, 4), (2, 8)), (0, 1, 4, 2.0), jnp.float32),
        "partial_key": gaussian_with(keys[1], (REPLICAS, WIDTH, ATTN), 0.5, 4.0, ((0, 4), (2, 8)), (0, 1, 4, 2.0), jnp.float32),
        "partial_value": gaussian_with(keys[2], (REPLICAS, WIDTH, ATTN), 0.5, 4.0, ((0, 4), (2, 8)), (0, 1, 4, 2.0), jnp.float32),
        "partial_mixed": gaussian_with(keys[3], (REPLICAS, ATTN, WIDTH), 0.5, 4.0, ((0, 4), (1, 8)), (0, 2, 4, 2.0), jnp.float32),
        "partial_norm": gaussian_with(keys[4], (REPLICAS, WIDTH), 1.0, 8.0, ((0, 4),), (0, 1, 4, 2.0), jnp.float32),
        "partial_bias": gaussian_with(keys[5], (REPLICAS, WIDTH), 1.0, 8.0, ((0, 4),), (0, 1, 4, 2.0), jnp.float32),
        "master_query": gaussian_with(keys[6], (WIDTH, ATTN), WIDTH ** -0.5, 0.1875, ((0, 4), (1, 8)), (1, 0, 8, 2.0), jnp.float32),
        "master_key": gaussian_with(keys[7], (WIDTH, ATTN), WIDTH ** -0.5, 0.1875, ((0, 4), (1, 8)), (1, 0, 8, 2.0), jnp.float32),
        "master_value": gaussian_with(keys[8], (WIDTH, ATTN), WIDTH ** -0.5, 0.1875, ((0, 4), (1, 8)), (1, 0, 8, 2.0), jnp.float32),
        "master_mixed": gaussian_with(keys[9], (ATTN, WIDTH), ATTN ** -0.5, 0.1875, ((0, 8), (1, 4)), (0, 1, 8, 2.0), jnp.float32),
        "master_norm": jnp.clip(1.0 + 0.15 * jax.random.normal(keys[10], (WIDTH,), jnp.float32), 0.25, 1.75),
        "master_bias": noise(keys[11], (WIDTH,), 0.5, 3.0, ((0, 4),), jnp.float32),
        "memory_query": jnp.clip(9.765625145519152e-05 + 0.0008789062 * jax.random.uniform(keys[12], (WIDTH, ATTN), jnp.float32) ** block_scale(keys[12], (WIDTH, ATTN), ((0, 4), (1, 8)), -0.2, 0.2), 9.765625145519152e-05, 0.0009765625),
        "memory_key": jnp.clip(9.765625145519152e-05 + 0.0008789062 * jax.random.uniform(keys[13], (WIDTH, ATTN), jnp.float32) ** block_scale(keys[13], (WIDTH, ATTN), ((0, 4), (1, 8)), -0.2, 0.2), 9.765625145519152e-05, 0.0009765625),
        "memory_value": jnp.clip(9.765625145519152e-05 + 0.0008789062 * jax.random.uniform(keys[14], (WIDTH, ATTN), jnp.float32) ** block_scale(keys[14], (WIDTH, ATTN), ((0, 4), (1, 8)), -0.2, 0.2), 9.765625145519152e-05, 0.0009765625),
        "memory_mixed": jnp.clip(9.765625145519152e-05 + 0.0008789062 * jax.random.uniform(keys[15], (ATTN, WIDTH), jnp.float32) ** block_scale(keys[15], (ATTN, WIDTH), ((0, 8), (1, 4)), -0.2, 0.2), 9.765625145519152e-05, 0.0009765625),
        "memory_norm": jnp.clip(0.05 + 0.75 * jax.random.uniform(keys[16], (WIDTH,), jnp.float32) ** block_scale(keys[16], (WIDTH,), ((0, 4),), -0.2, 0.2), 0.05, 0.8),
        "memory_bias": jnp.clip(0.05 + 0.75 * jax.random.uniform(keys[17], (WIDTH,), jnp.float32) ** block_scale(keys[17], (WIDTH,), ((0, 4),), -0.2, 0.2), 0.05, 0.8),
    }


learn_rate = 0.015
hold_rate = 0.8

def reference(partial_query, partial_key, partial_value, partial_mixed, partial_norm, partial_bias, master_query, master_key, master_value, master_mixed, master_norm, master_bias, memory_query, memory_key, memory_value, memory_mixed, memory_norm, memory_bias):
    mean_query = lax.optimization_barrier(jnp.sum(partial_query.astype(jnp.float32), axis=0)) * REPLICAS ** (-0.5)
    mean_key = lax.optimization_barrier(jnp.sum(partial_key.astype(jnp.float32), axis=0)) * REPLICAS ** (-0.5)
    mean_value = lax.optimization_barrier(jnp.sum(partial_value.astype(jnp.float32), axis=0)) * REPLICAS ** (-0.5)
    mean_mixed = lax.optimization_barrier(jnp.sum(partial_mixed.astype(jnp.float32), axis=0)) * REPLICAS ** (-0.5)
    mean_norm = lax.optimization_barrier(jnp.sum(partial_norm.astype(jnp.float32), axis=0)) * REPLICAS ** (-0.5)
    mean_bias = lax.optimization_barrier(jnp.sum(partial_bias.astype(jnp.float32), axis=0)) * REPLICAS ** (-0.5)
    ratio_query = jnp.sqrt(lax.optimization_barrier(jnp.sum(master_query * master_query, axis=1, keepdims=True))) * lax.rsqrt(lax.optimization_barrier(jnp.sum(mean_query * mean_query, axis=1, keepdims=True)) + 1e-06)
    mean_query = mean_query * ratio_query
    ratio_key = jnp.sqrt(lax.optimization_barrier(jnp.sum(master_key * master_key, axis=1, keepdims=True))) * lax.rsqrt(lax.optimization_barrier(jnp.sum(mean_key * mean_key, axis=1, keepdims=True)) + 1e-06)
    mean_key = mean_key * ratio_key
    ratio_value = jnp.sqrt(lax.optimization_barrier(jnp.sum(master_value * master_value, axis=1, keepdims=True))) * lax.rsqrt(lax.optimization_barrier(jnp.sum(mean_value * mean_value, axis=1, keepdims=True)) + 1e-06)
    mean_value = mean_value * ratio_value
    ratio_mixed = jnp.sqrt(lax.optimization_barrier(jnp.sum(master_mixed * master_mixed, axis=0, keepdims=True))) * lax.rsqrt(lax.optimization_barrier(jnp.sum(mean_mixed * mean_mixed, axis=0, keepdims=True)) + 1e-06)
    mean_mixed = mean_mixed * ratio_mixed
    state_new_query = hold_rate * memory_query + (1.0 - hold_rate) * mean_query * mean_query
    stepped_query = master_query - learn_rate * mean_query * lax.rsqrt(state_new_query + 1e-06)
    state_new_key = hold_rate * memory_key + (1.0 - hold_rate) * mean_key * mean_key
    stepped_key = master_key - learn_rate * mean_key * lax.rsqrt(state_new_key + 1e-06)
    state_new_value = hold_rate * memory_value + (1.0 - hold_rate) * mean_value * mean_value
    stepped_value = master_value - learn_rate * mean_value * lax.rsqrt(state_new_value + 1e-06)
    state_new_mixed = hold_rate * memory_mixed + (1.0 - hold_rate) * mean_mixed * mean_mixed
    stepped_mixed = master_mixed - learn_rate * mean_mixed * lax.rsqrt(state_new_mixed + 1e-06)
    state_new_norm = hold_rate * memory_norm + (1.0 - hold_rate) * mean_norm * mean_norm
    stepped_norm = master_norm - learn_rate * mean_norm * lax.rsqrt(state_new_norm + 1e-06)
    state_new_bias = hold_rate * memory_bias + (1.0 - hold_rate) * mean_bias * mean_bias
    stepped_bias = master_bias - learn_rate * mean_bias * lax.rsqrt(state_new_bias + 1e-06)
    compute_query = stepped_query.astype(jnp.bfloat16)
    compute_key = stepped_key.astype(jnp.bfloat16)
    compute_value = stepped_value.astype(jnp.bfloat16)
    compute_mixed = stepped_mixed.astype(jnp.bfloat16)
    compute_norm = stepped_norm.astype(jnp.bfloat16)
    compute_bias = stepped_bias.astype(jnp.bfloat16)
    return (compute_query, compute_key, compute_value, compute_mixed, compute_norm, compute_bias, stepped_query, stepped_key, stepped_value, stepped_mixed, stepped_norm, stepped_bias, state_new_query, state_new_key, state_new_value, state_new_mixed, state_new_norm, state_new_bias)
```

```python
import functools

import jax
import jax.numpy as jnp
from jax import lax
from jax.experimental import pallas as pl
from jax.experimental.pallas import tpu as pltpu
from jax.sharding import PartitionSpec as P

learn_rate = 0.015
hold_rate = 0.8
CORES = 2
AXES = (0, 0, 0, 1)


def cut(ref, axis, start, size):
    where = pl.ds(pl.multiple_of(start, 128), size)
    return ref.at[where, :] if axis == 0 else ref.at[:, where]


def update(mean, master, memory):
    state = hold_rate * memory + (1.0 - hold_rate) * mean * mean
    return master - learn_rate * mean * lax.rsqrt(state + 1e-06), state


def kernel(replicas, models, length, width, *refs):
    n = len(AXES)
    partial, vec_partial = refs[0:4], refs[4:6]
    master_in, vec_master = refs[6:10], refs[10:12]
    memory_in, vec_memory = refs[12:16], refs[16:18]
    compute_out, vec_compute = refs[18:22], refs[22:24]
    stepped_out, vec_stepped = refs[24:28], refs[28:30]
    state_out, vec_state = refs[30:34], refs[34:36]
    (own_r, own_c, sib_r, sib_c, rem_r, rem_c, mas_r, mas_c, mem_r, mem_c, comp_r, comp_c,
     far_r, far_c, near_r, near_c, squares, ratios, norms,
     vpart, vfull, vcomp,
     load_sem, near_send, near_recv, far_send, far_recv, norm_send, norm_recv,
     ag_send, ag_recv, sib_send, sib_recv, out_sem, vload_sem, vsend_sem, vrecv_sem, vout_sem) = refs[36:]
    chips = replicas // CORES
    place = lax.axis_index("replica")
    part = lax.axis_index("model")
    chip, core = place // CORES, place % CORES
    sibling = chip * CORES + (CORES - 1 - core)
    rate = replicas ** (-0.5)

    def at(row_ref, col_ref, i, *index):
        return row_ref.at[(i,) + index] if AXES[i] == 0 else col_ref.at[index]

    def to_replica(r):
        return {"replica": r, "model": part}

    def to_model(m):
        return {"replica": place, "model": m}

    def remote(src, dst, send, recv, device):
        return pltpu.make_async_remote_copy(
            src_ref=src, dst_ref=dst, send_sem=send, recv_sem=recv,
            device_id=device, device_id_type=pl.DeviceIdType.MESH)

    def chip_at(d):
        return lax.rem(chip + d, chips)

    order = list(range(1, chips)) + [0]
    loads = {}
    for i in range(n):
        for d in order:
            loads[i, d] = pltpu.make_async_copy(
                cut(partial[i].at[0], AXES[i], (chip_at(d) * CORES + core) * length, length),
                at(own_r, own_c, i, d), load_sem.at[i, d])
            loads[i, d].start()
    for i in range(n):
        for name, src, rows, cols, k in (("master", master_in, mas_r, mas_c, 0), ("memory", memory_in, mem_r, mem_c, 1)):
            loads[i, name] = pltpu.make_async_copy(src[i], at(rows, cols, i), load_sem.at[i, chips + k])
            loads[i, name].start()

    barrier = pltpu.get_barrier_semaphore()
    for d in range(1, replicas):
        pl.semaphore_signal(barrier, inc=1, device_id=to_replica(lax.rem(place + d, replicas)),
                            device_id_type=pl.DeviceIdType.MESH)
    for d in range(1, models):
        pl.semaphore_signal(barrier, inc=1, device_id=to_model(lax.rem(part + d, models)),
                            device_id_type=pl.DeviceIdType.MESH)
    pl.semaphore_wait(barrier, replicas - 1 + models - 1)

    near = {}
    for i in range(n):
        for d in order:
            near[i, d] = remote(
                cut(partial[i].at[0], AXES[i], (chip_at(d) * CORES + (CORES - 1 - core)) * length, length),
                at(sib_r, sib_c, i, d), near_send.at[i, d], near_recv.at[i, d], to_replica(sibling))
            near[i, d].start()

    mine = pl.ds(pl.multiple_of(place * length, 128), length)
    vsrc = [vec_partial[0], vec_partial[1], vec_master[0], vec_master[1], vec_memory[0], vec_memory[1]]
    vcopies = []
    for d in range(replicas):
        for k in range(6):
            dst = vpart.at[k, d] if k < 2 else vfull.at[k - 2, :, mine]
            if d == 0:
                c = pltpu.make_async_copy(vsrc[k], dst, vload_sem.at[k])
            else:
                c = remote(vsrc[k], dst, vsend_sem.at[d - 1, k], vrecv_sem.at[d - 1, k],
                           to_replica(lax.rem(place + d, replicas)))
            c.start()
            vcopies.append(c)

    def step_rows(i):
        return 64 if AXES[i] == 0 else 32

    def each(i, body, init=None):
        rows = length if AXES[i] == 0 else width
        step = step_rows(i)

        def run(j, carry):
            return body(pl.ds(pl.multiple_of(j * step, step), step), carry)

        return lax.fori_loop(0, rows // step, run, init)

    def add_sibling(i, d):
        loads[i, d].wait()
        near[i, d].wait_recv()
        own, sib = at(own_r, own_c, i, d), at(sib_r, sib_c, i, d)

        def body(rows, carry):
            own[rows, :] = own[rows, :] + sib[rows, :]
            return carry

        each(i, body, 0)

    far = {}
    for i in range(n):
        for d in range(1, chips):
            add_sibling(i, d)
            far[i, d] = remote(
                at(own_r, own_c, i, d), at(rem_r, rem_c, i, d - 1), far_send.at[i, d - 1], far_recv.at[i, d - 1],
                to_replica(chip_at(d) * CORES + core))
            far[i, d].start()

    lanes = lax.broadcasted_iota(jnp.int32, (64, 128), 1)
    for i in range(n):
        add_sibling(i, 0)
        loads[i, "master"].wait()
        loads[i, "memory"].wait()
        master = at(mas_r, mas_c, i)
        if AXES[i] == 0:
            def body(rows, carry, master=master, i=i):
                v = master[rows, :]
                squares[i, rows, :] = jnp.broadcast_to(jnp.sum(v * v, axis=1, keepdims=True), (64, 128))
                return carry

            each(i, body, 0)
        else:
            def body(rows, carry, master=master):
                v = master[rows, :]
                return carry + jnp.sum(v * v, axis=0, keepdims=True)

            own_mixed = each(i, body, jnp.zeros((1, length), jnp.float32))
            norms[i, 0] = jnp.broadcast_to(own_mixed, (8, length))

    for c in vcopies:
        c.wait()
    vouts = []
    for k in range(2):
        total = vpart[k, 0]
        for d in range(1, replicas):
            total = total + vpart[k, d]
        stepped, state = update(total * rate, vfull[k], vfull[2 + k])
        vfull[k] = stepped
        vfull[2 + k] = state
        vcomp[k] = stepped.astype(jnp.bfloat16)
        vouts.append(pltpu.make_async_copy(vcomp.at[k], vec_compute[k], vout_sem.at[k]))
        vouts.append(pltpu.make_async_copy(vfull.at[k, :, mine], vec_stepped[k], vout_sem.at[2 + k]))
        vouts.append(pltpu.make_async_copy(vfull.at[2 + k, :, mine], vec_state[k], vout_sem.at[4 + k]))
    for c in vouts:
        c.start()

    outs = list(vouts)
    sends = []
    gather, give = {}, {}
    for i in range(n):
        for d in range(1, chips):
            far[i, d].wait_recv()
        own = at(own_r, own_c, i, 0)
        rem = [at(rem_r, rem_c, i, d) for d in range(chips - 1)]

        def mean_of(rows, own=own, rem=rem):
            total = own[rows, :]
            for r in rem:
                total = total + r[rows, :]
            total = total * rate
            own[rows, :] = total
            return total

        if AXES[i] == 0:
            def body(rows, carry, i=i, mean_of=mean_of):
                v = mean_of(rows)
                slope = jnp.broadcast_to(jnp.sum(v * v, axis=1, keepdims=True), (64, 128))
                squares[i, rows, :] = jnp.where(lanes == 1, slope, squares[i, rows, :])
                return carry

            each(i, body, 0)
            norms[i, 0] = squares[i].T[0:8]
        else:
            def body(rows, carry, mean_of=mean_of):
                v = mean_of(rows)
                return carry + jnp.sum(v * v, axis=0, keepdims=True)

            slope = each(i, body, jnp.zeros((1, length), jnp.float32))
            row = lax.broadcasted_iota(jnp.int32, (8, length), 0)
            norms[i, 0] = jnp.where(row == 1, jnp.broadcast_to(slope, (8, length)), norms[i, 0])
        passed = []
        for d in range(1, models):
            c = remote(norms.at[i, 0], norms.at[i, d], norm_send.at[i, d - 1], norm_recv.at[i, d - 1],
                       to_model(lax.rem(part + d, models)))
            c.start()
            passed.append(c)
        for c in passed:
            c.wait_recv()
        total = norms[i, 0]
        for d in range(1, models):
            total = total + norms[i, d]
        ratio = jnp.sqrt(total[0:1]) * lax.rsqrt(total[1:2] + 1e-06)
        for c in passed:
            c.wait_send()
        if AXES[i] == 0:
            ratios[i] = jnp.broadcast_to(ratio, (128, length)).T

        master, memory, comp = at(mas_r, mas_c, i), at(mem_r, mem_c, i), at(comp_r, comp_c, i)

        def body(rows, carry, i=i, ratio=ratio, own=own, master=master, memory=memory, comp=comp):
            scale = ratios[i, rows, 0:1] if AXES[i] == 0 else ratio
            stepped, state = update(own[rows, :] * scale, master[rows, :], memory[rows, :])
            master[rows, :] = stepped
            memory[rows, :] = state
            comp[rows, :] = stepped.astype(jnp.bfloat16)
            return carry

        each(i, body, 0)
        for d in range(1, chips):
            gather[i, d] = remote(comp, at(far_r, far_c, i, d - 1), ag_send.at[i, d - 1], ag_recv.at[i, d - 1],
                                  to_replica(chip_at(d) * CORES + core))
            gather[i, d].start()
        give[i, 0] = remote(comp, at(near_r, near_c, i, 0), sib_send.at[i, 0], sib_recv.at[i, 0], to_replica(sibling))
        give[i, 0].start()
        for k, c in enumerate((
                pltpu.make_async_copy(comp, cut(compute_out[i], AXES[i], place * length, length), out_sem.at[i, 0]),
                pltpu.make_async_copy(master, stepped_out[i], out_sem.at[i, 1]),
                pltpu.make_async_copy(memory, state_out[i], out_sem.at[i, 2]))):
            c.start()
            outs.append(c)

    def write(i, buffer, r, k):
        c = pltpu.make_async_copy(buffer, cut(compute_out[i], AXES[i], r * length, length), out_sem.at[i, k])
        c.start()
        outs.append(c)

    for i in range(n):
        for d in range(1, chips):
            gather[i, d].wait_recv()
            buffer = at(far_r, far_c, i, d - 1)
            give[i, d] = remote(buffer, at(near_r, near_c, i, d), sib_send.at[i, d], sib_recv.at[i, d], to_replica(sibling))
            give[i, d].start()
            write(i, buffer, chip_at(chips - d) * CORES + core, 2 + d)
        give[i, 0].wait_recv()
        write(i, at(near_r, near_c, i, 0), sibling, 2 + chips)
    for i in range(n):
        for d in range(1, chips):
            give[i, d].wait_recv()
            write(i, at(near_r, near_c, i, d), chip_at(chips - d) * CORES + (CORES - 1 - core), 2 + chips + d)
    for group in (near, far, gather, give):
        for c in group.values():
            c.wait_send()
    for c in outs:
        c.wait()


def shards(*args):
    replicas, models = lax.axis_size("replica"), lax.axis_size("model")
    chips = replicas // CORES
    args = list(args)
    for k in (10, 11, 16, 17):
        args[k] = args[k].reshape(1, -1)
    length, width = args[6].shape
    n, rows = len(AXES), sum(a == 0 for a in AXES)
    f32, bf16 = jnp.float32, jnp.bfloat16
    total = length * replicas
    row, col = (length, width), (width, length)
    outs = []
    for a in AXES:
        outs.append(jax.ShapeDtypeStruct((total, width) if a == 0 else (width, total), bf16))
    outs += [jax.ShapeDtypeStruct((1, total), bf16)] * 2
    one = [jax.ShapeDtypeStruct(row if a == 0 else col, f32) for a in AXES]
    one += [jax.ShapeDtypeStruct((1, length), f32)] * 2
    outs += one + one
    dma = pltpu.SemaphoreType.DMA
    scratch = []
    for lead, kind in ((chips, f32), (chips, f32), (chips - 1, f32), (None, f32), (None, f32), (None, bf16),
                       (chips - 1, bf16), (chips, bf16)):
        more = () if lead is None else (lead,)
        scratch += [pltpu.VMEM((rows,) + more + row, kind), pltpu.VMEM(more + col, kind)]
    scratch += [
        pltpu.VMEM((rows, length, 128), f32),
        pltpu.VMEM((rows, length, 128), f32),
        pltpu.VMEM((n, models, 8, length), f32),
        pltpu.VMEM((2, replicas, 1, total), f32),
        pltpu.VMEM((4, 1, total), f32),
        pltpu.VMEM((2, 1, total), bf16),
        dma((n, chips + 2)), dma((n, chips)), dma((n, chips)), dma((n, chips - 1)), dma((n, chips - 1)),
        dma((n, models - 1)), dma((n, models - 1)),
        dma((n, chips - 1)), dma((n, chips - 1)), dma((n, chips)), dma((n, chips)),
        dma((n, 2 + 2 * chips)), dma((6,)), dma((replicas - 1, 6)), dma((replicas - 1, 6)), dma((6,)),
    ]
    anywhere = pl.BlockSpec(memory_space=pl.ANY)
    result = pl.pallas_call(
        functools.partial(kernel, replicas, models, length, width),
        out_shape=outs,
        in_specs=[anywhere] * len(args),
        out_specs=[anywhere] * len(outs),
        scratch_shapes=scratch,
        compiler_params=pltpu.CompilerParams(collective_id=0, has_side_effects=True),
    )(*args)
    result = list(result)
    for k in (4, 5, 10, 11, 16, 17):
        result[k] = result[k].reshape(-1)
    return tuple(result)


def solution(mesh):
    ins = [P("replica", None, "model")] * 3 + [P("replica", "model", None)] + [P("replica", None)] * 2
    held = [P("replica", "model")] * 3 + [P("model", "replica")] + [P("replica")] * 2
    whole = [P(None, "model")] * 3 + [P("model", None)] + [P()] * 2
    return jax.shard_map(shards, mesh=mesh, in_specs=tuple(ins + held + held),
                         out_specs=tuple(whole + held + held), check_vma=False)
```

```python
import functools

import jax
import jax.numpy as jnp
from jax import lax
from jax.experimental import pallas as pl
from jax.experimental.pallas import tpu as pltpu
from jax.sharding import PartitionSpec as P

learn_rate = 0.015
hold_rate = 0.8
CORES = 2
AXES = (0, 0, 0, 1)


def cut(ref, axis, start, size):
    where = pl.ds(pl.multiple_of(start, 128), size)
    return ref.at[where, :] if axis == 0 else ref.at[:, where]


REACH = 4.0
SCALE = 2.0**15 / (CORES * REACH)


def encode(x):
    t = x * SCALE
    square = t * t
    return (square * square * square * (t * jnp.abs(t))).astype(jnp.bfloat16)


def decode(y):
    y = y.astype(jnp.float32)
    fourth = lax.rsqrt(lax.rsqrt(jnp.maximum(jnp.abs(y), 2.0**-126)))
    root = fourth * lax.rsqrt(fourth) * (1.0 / SCALE)
    return jnp.where(y > 0.0, root, jnp.where(y < 0.0, -root, 0.0))


def update(mean, master, memory):
    state = hold_rate * memory + (1.0 - hold_rate) * mean * mean
    return master - learn_rate * mean * lax.rsqrt(state + 1e-06), state


def kernel(replicas, models, length, width, *refs):
    n = len(AXES)
    partial, vec_partial = refs[0:4], refs[4:6]
    master_in, vec_master = refs[6:10], refs[10:12]
    memory_in, vec_memory = refs[12:16], refs[16:18]
    compute_out, vec_compute = refs[18:22], refs[22:24]
    stepped_out, vec_stepped = refs[24:28], refs[28:30]
    state_out, vec_state = refs[30:34], refs[34:36]
    (own_r, own_c, sib_r, sib_c, code_r, code_c, rem_r, rem_c, full_r, full_c, mas_r, mas_c, mem_r, mem_c, comp_r, comp_c,
     far_r, far_c, near_r, near_c, squares, ratios, norms,
     vpart, vfull,
     load_sem, near_send, near_recv, far_send, far_recv, norm_send, norm_recv,
     ag_send, ag_recv, sib_send, sib_recv, out_sem, vload_sem, vsend_sem, vrecv_sem, vout_sem) = refs[36:]
    chips = replicas // CORES
    place = lax.axis_index("replica")
    part = lax.axis_index("model")
    chip, core = place // CORES, place % CORES
    sibling = chip * CORES + (CORES - 1 - core)
    rate = replicas ** (-0.5)

    def at(row_ref, col_ref, i, *index):
        return row_ref.at[(i,) + index] if AXES[i] == 0 else col_ref.at[index]

    def to_replica(r):
        return {"replica": r, "model": part}

    def to_model(m):
        return {"replica": place, "model": m}

    def remote(src, dst, send, recv, device):
        return pltpu.make_async_remote_copy(
            src_ref=src, dst_ref=dst, send_sem=send, recv_sem=recv,
            device_id=device, device_id_type=pl.DeviceIdType.MESH)

    def chip_at(d):
        return lax.rem(chip + d, chips)

    order = list(range(1, chips)) + [0]
    loads = {}
    for i in range(n):
        for d in order:
            loads[i, d] = pltpu.make_async_copy(
                cut(partial[i].at[0], AXES[i], (chip_at(d) * CORES + core) * length, length),
                at(own_r, own_c, i, d), load_sem.at[i, d])
            loads[i, d].start()
    for i in range(n):
        for name, src, rows, cols, k in (("master", master_in, mas_r, mas_c, 0), ("memory", memory_in, mem_r, mem_c, 1)):
            loads[i, name] = pltpu.make_async_copy(src[i], at(rows, cols, i), load_sem.at[i, chips + k])
            loads[i, name].start()

    barrier = pltpu.get_barrier_semaphore()
    for d in range(1, replicas):
        pl.semaphore_signal(barrier, inc=1, device_id=to_replica(lax.rem(place + d, replicas)),
                            device_id_type=pl.DeviceIdType.MESH)
    for d in range(1, models):
        pl.semaphore_signal(barrier, inc=1, device_id=to_model(lax.rem(part + d, models)),
                            device_id_type=pl.DeviceIdType.MESH)
    pl.semaphore_wait(barrier, replicas - 1 + models - 1)

    near = {}
    for i in range(n):
        for d in order:
            near[i, d] = remote(
                cut(partial[i].at[0], AXES[i], (chip_at(d) * CORES + (CORES - 1 - core)) * length, length),
                at(sib_r, sib_c, i, d), near_send.at[i, d], near_recv.at[i, d], to_replica(sibling))
            near[i, d].start()

    mine = pl.ds(pl.multiple_of(place * length, 128), length)
    vsrc = [vec_partial[0], vec_partial[1], vec_master[0], vec_master[1], vec_memory[0], vec_memory[1]]
    vcopies = []
    for d in range(replicas):
        for k in range(6):
            dst = vpart.at[k, d] if k < 2 else vfull.at[k - 2, :, mine]
            if d == 0:
                c = pltpu.make_async_copy(vsrc[k], dst, vload_sem.at[k])
            else:
                c = remote(vsrc[k], dst, vsend_sem.at[d - 1, k], vrecv_sem.at[d - 1, k],
                           to_replica(lax.rem(place + d, replicas)))
            c.start()
            vcopies.append(c)

    def step_rows(i):
        return 64 if AXES[i] == 0 else 32

    def half(i):
        return (length if AXES[i] == 0 else width) // 2

    def each(i, body, init=None, parts=(0, 1)):
        step = step_rows(i)

        def run(j, carry):
            return body(pl.ds(pl.multiple_of(j * step, step), step), carry)

        start, stop = parts[0] * half(i), (parts[-1] + 1) * half(i)
        return lax.fori_loop(start // step, stop // step, run, init)

    def add_sibling(i, d):
        loads[i, d].wait()
        near[i, d].wait_recv()
        own, sib = at(own_r, own_c, i, d), at(sib_r, sib_c, i, d)
        code = at(code_r, code_c, i, d - 1) if d > 0 else None

        def whole(rows, carry):
            own[rows, :] = own[rows, :] + sib[rows, :]
            return carry

        def coded(rows, carry):
            code[rows, :] = encode(own[rows, :] + sib[rows, :])
            return carry

        if d > 0:
            each(i, coded, 0, (0,))
            each(i, whole, 0, (1,))
        else:
            each(i, whole, 0)

    far = {}
    for i in range(n):
        for d in range(1, chips):
            add_sibling(i, d)
            lower = pl.ds(half(i), half(i))
            for k, (src, dst) in enumerate((
                    (at(code_r, code_c, i, d - 1), at(rem_r, rem_c, i, d - 1)),
                    (at(own_r, own_c, i, d).at[lower, :], at(full_r, full_c, i, d - 1)))):
                far[i, d, k] = remote(src, dst, far_send.at[i, d - 1, k], far_recv.at[i, d - 1, k],
                                      to_replica(chip_at(d) * CORES + core))
                far[i, d, k].start()

    lanes = lax.broadcasted_iota(jnp.int32, (64, 128), 1)
    for i in range(n):
        add_sibling(i, 0)
        loads[i, "master"].wait()
        loads[i, "memory"].wait()
        master = at(mas_r, mas_c, i)
        if AXES[i] == 0:
            def body(rows, carry, master=master, i=i):
                v = master[rows, :]
                squares[i, rows, :] = jnp.broadcast_to(jnp.sum(v * v, axis=1, keepdims=True), (64, 128))
                return carry

            each(i, body, 0)
        else:
            def body(rows, carry, master=master):
                v = master[rows, :]
                return carry + jnp.sum(v * v, axis=0, keepdims=True)

            own_mixed = each(i, body, jnp.zeros((1, length), jnp.float32))
            norms[i, 0] = jnp.broadcast_to(own_mixed, (8, length))

    for c in vcopies:
        c.wait()
    vouts = []
    for k in range(2):
        total = vpart[k, 0]
        for d in range(1, replicas):
            total = total + vpart[k, d]
        stepped, state = update(total * rate, vfull[k], vfull[2 + k])
        vfull[k] = stepped
        vfull[2 + k] = state
        vouts.append(pltpu.make_async_copy(vfull.at[k], vec_compute[k], vout_sem.at[k]))
        vouts.append(pltpu.make_async_copy(vfull.at[k, :, mine], vec_stepped[k], vout_sem.at[2 + k]))
        vouts.append(pltpu.make_async_copy(vfull.at[2 + k, :, mine], vec_state[k], vout_sem.at[4 + k]))
    for c in vouts:
        c.start()

    outs = list(vouts)
    sends = []
    gather, give = {}, {}
    for i in range(n):
        for d in range(1, chips):
            far[i, d, 0].wait_recv()
            far[i, d, 1].wait_recv()
        own = at(own_r, own_c, i, 0)
        rem = [at(rem_r, rem_c, i, d) for d in range(chips - 1)]
        full = [at(full_r, full_c, i, d) for d in range(chips - 1)]

        def add_coded(rows, carry, own=own, rem=rem):
            total = own[rows, :]
            for r in rem:
                total = total + decode(r[rows, :])
            own[rows, :] = total
            return carry

        def add_full(rows, carry, own=own, full=full, i=i):
            there = pl.ds(pl.multiple_of(rows.start - half(i), step_rows(i)), step_rows(i))
            total = own[rows, :]
            for r in full:
                total = total + r[there, :]
            own[rows, :] = total
            return carry

        each(i, add_coded, 0, (0,))
        each(i, add_full, 0, (1,))

        def mean_of(rows, own=own):
            total = own[rows, :] * rate
            own[rows, :] = total
            return total

        if AXES[i] == 0:
            def body(rows, carry, i=i, mean_of=mean_of):
                v = mean_of(rows)
                slope = jnp.broadcast_to(jnp.sum(v * v, axis=1, keepdims=True), (64, 128))
                squares[i, rows, :] = jnp.where(lanes == 1, slope, squares[i, rows, :])
                return carry

            each(i, body, 0)
            norms[i, 0] = squares[i].T[0:8]
        else:
            def body(rows, carry, mean_of=mean_of):
                v = mean_of(rows)
                return carry + jnp.sum(v * v, axis=0, keepdims=True)

            slope = each(i, body, jnp.zeros((1, length), jnp.float32))
            row = lax.broadcasted_iota(jnp.int32, (8, length), 0)
            norms[i, 0] = jnp.where(row == 1, jnp.broadcast_to(slope, (8, length)), norms[i, 0])
        passed = []
        for d in range(1, models):
            c = remote(norms.at[i, 0], norms.at[i, d], norm_send.at[i, d - 1], norm_recv.at[i, d - 1],
                       to_model(lax.rem(part + d, models)))
            c.start()
            passed.append(c)
        for c in passed:
            c.wait_recv()
        total = norms[i, 0]
        for d in range(1, models):
            total = total + norms[i, d]
        ratio = jnp.sqrt(total[0:1]) * lax.rsqrt(total[1:2] + 1e-06)
        for c in passed:
            c.wait_send()
        if AXES[i] == 0:
            ratios[i] = jnp.broadcast_to(ratio, (128, length)).T

        master, memory, comp = at(mas_r, mas_c, i), at(mem_r, mem_c, i), at(comp_r, comp_c, i)

        def body(rows, carry, i=i, ratio=ratio, own=own, master=master, memory=memory, comp=comp):
            scale = ratios[i, rows, 0:1] if AXES[i] == 0 else ratio
            stepped, state = update(own[rows, :] * scale, master[rows, :], memory[rows, :])
            master[rows, :] = stepped
            memory[rows, :] = state
            comp[rows, :] = stepped.astype(jnp.bfloat16)
            return carry

        each(i, body, 0)
        for d in range(1, chips):
            gather[i, d] = remote(comp, at(far_r, far_c, i, d - 1), ag_send.at[i, d - 1], ag_recv.at[i, d - 1],
                                  to_replica(chip_at(d) * CORES + core))
            gather[i, d].start()
        give[i, 0] = remote(comp, at(near_r, near_c, i, 0), sib_send.at[i, 0], sib_recv.at[i, 0], to_replica(sibling))
        give[i, 0].start()
        for k, c in enumerate((
                pltpu.make_async_copy(comp, cut(compute_out[i], AXES[i], place * length, length), out_sem.at[i, 0]),
                pltpu.make_async_copy(master, stepped_out[i], out_sem.at[i, 1]),
                pltpu.make_async_copy(memory, state_out[i], out_sem.at[i, 2]))):
            c.start()
            outs.append(c)

    def write(i, buffer, r, k):
        c = pltpu.make_async_copy(buffer, cut(compute_out[i], AXES[i], r * length, length), out_sem.at[i, k])
        c.start()
        outs.append(c)

    for i in range(n):
        for d in range(1, chips):
            gather[i, d].wait_recv()
            buffer = at(far_r, far_c, i, d - 1)
            give[i, d] = remote(buffer, at(near_r, near_c, i, d), sib_send.at[i, d], sib_recv.at[i, d], to_replica(sibling))
            give[i, d].start()
            write(i, buffer, chip_at(chips - d) * CORES + core, 2 + d)
        give[i, 0].wait_recv()
        write(i, at(near_r, near_c, i, 0), sibling, 2 + chips)
    for i in range(n):
        for d in range(1, chips):
            give[i, d].wait_recv()
            write(i, at(near_r, near_c, i, d), chip_at(chips - d) * CORES + (CORES - 1 - core), 2 + chips + d)
    for group in (near, far, gather, give):
        for c in group.values():
            c.wait_send()
    for c in outs:
        c.wait()


def write_out(count, *refs):
    source, target, held = refs[:count], refs[count:2 * count], refs[2 * count:3 * count]
    in_sem, out_sem = refs[3 * count:]
    reads = [pltpu.make_async_copy(a, b, in_sem.at[k]) for k, (a, b) in enumerate(zip(source, held))]
    writes = [pltpu.make_async_copy(a, b, out_sem.at[k]) for k, (a, b) in enumerate(zip(held, target))]
    for c in reads:
        c.start()
    for read, c in zip(reads, writes):
        read.wait()
        c.start()
    for c in writes:
        c.wait()


def shards(*args):
    replicas, models = lax.axis_size("replica"), lax.axis_size("model")
    chips = replicas // CORES
    args = list(args)
    for k in (10, 11, 16, 17):
        args[k] = args[k].reshape(1, -1)
    length, width = args[6].shape
    n, rows = len(AXES), sum(a == 0 for a in AXES)
    f32, bf16 = jnp.float32, jnp.bfloat16
    total = length * replicas
    row, col = (length, width), (width, length)
    outs = []
    for a in AXES:
        outs.append(jax.ShapeDtypeStruct((total, width) if a == 0 else (width, total), bf16))
    outs += [jax.ShapeDtypeStruct((1, total), f32)] * 2
    one = [jax.ShapeDtypeStruct(row if a == 0 else col, f32) for a in AXES]
    one += [jax.ShapeDtypeStruct((1, length), f32)] * 2
    outs += one + one
    dma = pltpu.SemaphoreType.DMA
    scratch = []
    for lead, kind in ((chips, f32), (chips, f32), (1 - chips, bf16), (1 - chips, bf16), (1 - chips, f32), (None, f32), (None, f32), (None, bf16),
                       (chips - 1, bf16), (chips, bf16)):
        more, cuts = ((), 1) if lead is None else ((abs(lead),), 2 if lead < 0 else 1)
        scratch += [pltpu.VMEM((rows,) + more + (length // cuts, width), kind),
                    pltpu.VMEM(more + (width // cuts, length), kind)]
    scratch += [
        pltpu.VMEM((rows, length, 128), f32),
        pltpu.VMEM((rows, length, 128), f32),
        pltpu.VMEM((n, models, 8, length), f32),
        pltpu.VMEM((2, replicas, 1, total), f32),
        pltpu.VMEM((4, 1, total), f32),
        dma((n, chips + 2)), dma((n, chips)), dma((n, chips)), dma((n, chips - 1, 2)), dma((n, chips - 1, 2)),
        dma((n, models - 1)), dma((n, models - 1)),
        dma((n, chips - 1)), dma((n, chips - 1)), dma((n, chips)), dma((n, chips)),
        dma((n, 2 + 2 * chips)), dma((6,)), dma((replicas - 1, 6)), dma((replicas - 1, 6)), dma((6,)),
    ]
    anywhere = pl.BlockSpec(memory_space=pl.ANY)
    result = pl.pallas_call(
        functools.partial(kernel, replicas, models, length, width),
        out_shape=outs,
        in_specs=[anywhere] * len(args),
        out_specs=[anywhere] * len(outs),
        scratch_shapes=scratch,
        compiler_params=pltpu.CompilerParams(collective_id=0, has_side_effects=True),
    )(*args)
    result = list(result)
    picks = [k for k in range(len(outs)) if k not in (4, 5)][::-1]
    shapes = [outs[k] for k in picks]
    placed = pl.pallas_call(
        functools.partial(write_out, len(picks)),
        out_shape=shapes,
        in_specs=[anywhere] * len(picks),
        out_specs=[anywhere] * len(picks),
        scratch_shapes=[pltpu.VMEM(a.shape, a.dtype) for a in shapes] + [dma((len(picks),)), dma((len(picks),))],
    )(*[result[k] for k in picks])
    for k, a in zip(picks, placed):
        result[k] = a
    for k in (4, 5, 10, 11, 16, 17):
        result[k] = result[k].reshape(-1)
    for k in (4, 5):
        result[k] = result[k].astype(bf16)
    return tuple(result)


def solution(mesh):
    ins = [P("replica", None, "model")] * 3 + [P("replica", "model", None)] + [P("replica", None)] * 2
    held = [P("replica", "model")] * 3 + [P("model", "replica")] + [P("replica")] * 2
    whole = [P(None, "model")] * 3 + [P("model", None)] + [P()] * 2
    return jax.shard_map(shards, mesh=mesh, in_specs=tuple(ins + held + held),
                         out_specs=tuple(whole + held + held), check_vma=False)
```
